32 devices in a mesh: data: 2 (over x), inner: 4 (over z), stage: 4 (over y, core).
Axes of the slice: x: 2, y: 2, z: 4, core: 2. Of those that a mesh axis runs over, the one named last changes fastest.
Arguments:
- x_tokens: bfloat16 [32, 256, 768], P(('data', 'stage', 'inner')), parts along dimension 0
- g_cotan: bfloat16 [32, 256, 768], P(('data', 'stage', 'inner')), parts along dimension 0
- w_up: bfloat16 [2, 8, 768, 3072], P(None, ('data', 'stage'), None, 'inner'), parts along dimension 1
- w_down: bfloat16 [2, 8, 3072, 768], P(None, ('data', 'stage'), 'inner'), parts along dimension 1
Outputs:
- output 1: bfloat16 [32, 256, 768], P(('data', 'stage', 'inner')), parts along dimension 0
- output 2: bfloat16 [32, 256, 768], P(('data', 'stage', 'inner')), parts along dimension 0
- output 3: float32 [2, 8, 768, 3072], P(None, ('data', 'stage'), None, 'inner'), parts along dimension 1
- output 4: float32 [2, 8, 3072, 768], P(None, ('data', 'stage'), 'inner'), parts along dimension 1
There are 2 independent parts. The reference program is written for one: setup_inputs(seed, part) draws one part's arguments, and reference() takes and returns one part's arrays. A program takes and returns all parts, laid end to end along the dimension named above; each array names one.
All inputs are finite; a program needn't handle non-finite values.
Results may differ from the reference program's by a relative error of at most 0.0161341.
Values are sent between devices in bfloat16 or wider.
A program may use at most 1 GiB of HBM per device.

```python
import jax
import jax.numpy as jnp
from jax import lax

D_MODEL = 768
D_FF = 3072
MB_TOKENS = 256
MB_PER_DEV = 1
VIRT_STAGES = 2
CHUNK_LAYERS = 1
NUM_STAGES = 4
INNER_SIZE = 4

NUM_MICRO = MB_PER_DEV * NUM_STAGES * INNER_SIZE
STAGE_LAYERS = NUM_STAGES * CHUNK_LAYERS
NUM_LAYERS = VIRT_STAGES * STAGE_LAYERS


def setup_inputs(seed: int = 0, part: int = 0) -> dict:
    base_key = jax.random.fold_in(jax.random.key(seed), part)
    key_list = jax.random.split(base_key, 4)
    tok_shape = (NUM_MICRO, MB_TOKENS, D_MODEL)
    x_tokens = jax.random.normal(key_list[0], tok_shape, jnp.float32)
    g_cotan = jax.random.normal(key_list[1], tok_shape, jnp.float32)
    up_scale = D_MODEL ** -0.5
    down_scale = 1.5 * (D_FF * NUM_LAYERS) ** -0.5
    w_up = jax.random.normal(key_list[2], (VIRT_STAGES, STAGE_LAYERS, D_MODEL, D_FF), jnp.float32) * up_scale
    w_down = jax.random.normal(key_list[3], (VIRT_STAGES, STAGE_LAYERS, D_FF, D_MODEL), jnp.float32) * down_scale
    return {'x_tokens': x_tokens.astype(jnp.bfloat16), 'g_cotan': g_cotan.astype(jnp.bfloat16), 'w_up': w_up.astype(jnp.bfloat16), 'w_down': w_down.astype(jnp.bfloat16)}


def gelu_pair(pre_act):
    normal_cdf = 0.5 * (1.0 + lax.erf(pre_act * 0.7071067811865476))
    normal_pdf = jnp.exp(-0.5 * pre_act * pre_act) * 0.3989422804014327
    return pre_act * normal_cdf, normal_cdf + pre_act * normal_pdf


def reference(x_tokens, g_cotan, w_up, w_down):
    up_layers = w_up.reshape(NUM_LAYERS, D_MODEL, D_FF)
    down_layers = w_down.reshape(NUM_LAYERS, D_FF, D_MODEL)

    def fwd_layer(h_act, weights):
        w_one, w_two = weights
        pre_act = jnp.dot(h_act, w_one, preferred_element_type=jnp.float32)
        act_val = gelu_pair(pre_act)[0].astype(jnp.bfloat16)
        branch = jnp.dot(act_val, w_two, preferred_element_type=jnp.float32)
        h_next = (h_act.astype(jnp.float32) + branch).astype(jnp.bfloat16)
        return h_next, h_act

    def bwd_layer(g_act, layer_items):
        h_in, w_one, w_two = layer_items
        pre_act = jnp.dot(h_in, w_one, preferred_element_type=jnp.float32)
        gelu_val, gelu_grad = gelu_pair(pre_act)
        act_val = gelu_val.astype(jnp.bfloat16)
        d_act = jnp.dot(g_act, w_two.T, preferred_element_type=jnp.float32)
        d_pre = (d_act * gelu_grad).astype(jnp.bfloat16)
        grad_one = jnp.dot(h_in.T, d_pre, preferred_element_type=jnp.float32)
        grad_two = jnp.dot(act_val.T, g_act, preferred_element_type=jnp.float32)
        back_term = jnp.dot(d_pre, w_one.T, preferred_element_type=jnp.float32)
        g_prev = (g_act.astype(jnp.float32) + back_term).astype(jnp.bfloat16)
        return g_prev, (grad_one, grad_two)

    def one_micro(acc_state, micro_items):
        x_micro, g_micro = micro_items
        y_micro, layer_ins = lax.scan(fwd_layer, x_micro, (up_layers, down_layers))
        dx_micro, grad_pair = lax.scan(bwd_layer, g_micro, (layer_ins, up_layers, down_layers), reverse=True)
        new_state = (acc_state[0] + grad_pair[0], acc_state[1] + grad_pair[1])
        return new_state, (y_micro, dx_micro)

    init_state = (jnp.zeros(up_layers.shape, jnp.float32), jnp.zeros(down_layers.shape, jnp.float32))
    final_state, micro_outs = lax.scan(one_micro, init_state, (x_tokens, g_cotan))
    dw_up = final_state[0].reshape(w_up.shape)
    dw_down = final_state[1].reshape(w_down.shape)
    return (micro_outs[0], micro_outs[1], dw_up, dw_down)
```

```python
import functools

import jax
import jax.numpy as jnp
from jax import lax
from jax.experimental import pallas as pl
from jax.experimental.pallas import tpu as pltpu
from jax.sharding import PartitionSpec as P

MESH = pl.DeviceIdType.MESH
F32 = jnp.float32
BF16 = jnp.bfloat16
N_CHIP = 8
N_BLK = 4


def gelu_only(z):
    return z * (0.5 * (1.0 + lax.erf(z * 0.7071067811865476)))


def gelu_pair(z):
    cdf = 0.5 * (1.0 + lax.erf(z * 0.7071067811865476))
    pdf = jnp.exp(-0.5 * z * z) * 0.3989422804014327
    return z * cdf, cdf + z * pdf


def dot_nn(a, b):
    return lax.dot_general(a, b, (((1,), (0,)), ((), ())), preferred_element_type=F32)


def dot_nt(a, b):
    return lax.dot_general(a, b, (((1,), (1,)), ((), ())), preferred_element_type=F32)


def dot_tn(a, b):
    return lax.dot_general(a, b, (((0,), (0,)), ((), ())), preferred_element_type=F32)


def chip_z(layer):
    return lax.rem(1 + (layer + 1) // 2, 4)


def chip_y(layer):
    return lax.rem(layer // 2, 2)


def kernel(x_ref, g_ref, wu_ref, wd_ref, y_ref, dx_ref, dwu_ref, dwd_ref,
           w_all, acc, pbuf, hbuf, hout, gbuf, gout, a_s, dz_s,
           x_send, g_send, w_send, w_recv, w_fwd, h_recv, g_recv, h_send, g_sent,
           y_recv, dx_recv, p_send, p_recv, dw_send, dw_recv):
    z = lax.axis_index("inner")
    s = lax.axis_index("stage")
    y = s // 2
    core = lax.rem(s, 2)
    par, half = lax.rem(z, 2), z // 2
    layer = (1 - y) * (5 - 5 * par - 4 * half + 8 * par * half) + y * (6 + par - 4 * half)
    n_chunk, rows, d = hbuf.shape
    partner = 2 * y + (1 - core)
    here = {"inner": z, "stage": s}

    def copy(src, dst, send, recv, dz, ds):
        return pltpu.make_async_remote_copy(
            src_ref=src, dst_ref=dst, send_sem=send, recv_sem=recv,
            device_id={"inner": dz, "stage": ds}, device_id_type=MESH)

    def arrived(slot, sem):
        copy(slot, slot, sem, sem, z, s).wait_recv()

    def sent(slot, sem):
        copy(slot, slot, sem, sem, z, s).wait_send()

    def push(src, dst, send, recv, dz, ds):
        same = (dz == z) & (ds == s)

        @pl.when(same)
        def _():
            pltpu.make_async_copy(src, dst, recv).start()

        @pl.when(jnp.logical_not(same))
        def _():
            copy(src, dst, send, recv, dz, ds).start()

    def pushed(src, send, dz, ds):
        @pl.when(jnp.logical_not((dz == z) & (ds == s)))
        def _():
            sent(src, send)

    def send_weights(v):
        tgt = chip_z(4 * v + s)
        push(wu_ref.at[v], w_all.at[0, z], w_send.at[v, 0], w_recv.at[0, z], tgt, 2 * y)
        push(wd_ref.at[v], w_all.at[1, z], w_send.at[v, 1], w_recv.at[1, z], tgt, 2 * y + 1)

    def weights_sent(v):
        tgt = chip_z(4 * v + s)
        pushed(wu_ref.at[v], w_send.at[v, 0], tgt, 2 * y)
        pushed(wd_ref.at[v], w_send.at[v, 1], tgt, 2 * y + 1)

    chip = 4 * y + z
    send_weights(0)
    for q in range(2):
        slot = 2 * chip + q
        push(x_ref.at[q], hbuf.at[slot], x_send.at[q], h_recv.at[slot], 1, core)
    for k in range(2):
        for b in range(N_BLK):
            acc[k, b] = jnp.zeros(acc.shape[2:], F32)
    weights_sent(0)
    send_weights(1)
    for q in range(2):
        slot = 2 * chip + q
        push(g_ref.at[q], gbuf.at[slot], g_send.at[q], g_recv.at[slot], 1, 2 + core)
    for b in range(N_BLK):
        arrived(w_all.at[core, b], w_recv.at[core, b])
        copy(w_all.at[core, b], w_all.at[core, b], w_fwd.at[b], w_recv.at[core, b], z, partner).start()
    for b in range(N_BLK):
        arrived(w_all.at[1 - core, b], w_recv.at[1 - core, b])

    nxt, prv = layer + 1, layer - 1
    last, first = layer == 7, layer == 0

    def forward(m, carry):
        arrived(hbuf.at[m], h_recv.at[m])
        h = hbuf[m]
        out = h.astype(F32)
        branch = jnp.zeros((rows, d), F32)
        for b in range(N_BLK):
            a = gelu_only(dot_nn(h, w_all[0, b])).astype(BF16)
            branch = branch + dot_nn(a, w_all[1, b])
        hout[m] = (out + branch).astype(BF16)

        @pl.when(layer < 7)
        def _():
            copy(hout.at[m], hbuf.at[m], h_send.at[m], h_recv.at[m],
                 chip_z(nxt), 2 * chip_y(nxt) + core).start()

        @pl.when(last)
        def _():
            home, q = m // 2, lax.rem(m, 2)
            push(hout.at[m], y_ref.at[q], h_send.at[m], y_recv.at[q],
                 lax.rem(home, 4), 2 * (home // 4) + core)
        return carry

    lax.fori_loop(0, n_chunk, forward, 0)

    def backward(p, carry):
        for q in range(2):
            m = 2 * p + q
            arrived(gbuf.at[m], g_recv.at[m])
            h = hbuf[m]
            g = gbuf[m]
            back = jnp.zeros((rows, d), F32)
            for b in range(N_BLK):
                act, grad = gelu_pair(dot_nn(h, w_all[0, b]))
                dz = (dot_nt(g, w_all[1, b]) * grad).astype(BF16)
                a_s[b, pl.ds(q * rows, rows), :] = act.astype(BF16)
                dz_s[b, pl.ds(q * rows, rows), :] = dz
                back = back + dot_nt(dz, w_all[0, b])
            gout[m] = (g.astype(F32) + back).astype(BF16)

            @pl.when(layer > 0)
            def _():
                copy(gout.at[m], gbuf.at[m], g_sent.at[m], g_recv.at[m],
                     chip_z(prv), 2 * chip_y(prv) + core).start()

            @pl.when(first)
            def _():
                push(gout.at[m], dx_ref.at[q], g_sent.at[m], dx_recv.at[q],
                     lax.rem(p, 4), 2 * (p // 4) + core)

        h2 = hbuf[pl.ds(2 * p, 2)].reshape(2 * rows, d)
        g2 = gbuf[pl.ds(2 * p, 2)].reshape(2 * rows, d)
        for b in range(N_BLK):
            acc[0, b] += dot_tn(h2, dz_s[b])
            acc[1, b] += dot_tn(a_s[b], g2)
        return carry

    lax.fori_loop(0, n_chunk // 2, backward, 0)

    for b in range(N_BLK):
        copy(acc.at[1 - core, b], pbuf.at[b], p_send.at[b], p_recv.at[b], z, partner).start()
    virt = layer // 4
    owner = lax.rem(layer, 4)
    for b in range(N_BLK):
        arrived(pbuf.at[b], p_recv.at[b])
        acc[core, b] += pbuf[b]

        @pl.when(core == 0)
        def _():
            push(acc.at[0, b], dwu_ref.at[virt], dw_send.at[b], dw_recv.at[0, virt], b, owner)

        @pl.when(core == 1)
        def _():
            push(acc.at[1, b], dwd_ref.at[virt], dw_send.at[b], dw_recv.at[1, virt], b, owner)

    for q in range(2):
        pushed(x_ref.at[q], x_send.at[q], 1, core)
        pushed(g_ref.at[q], g_send.at[q], 1, 2 + core)
        arrived(y_ref.at[q], y_recv.at[q])
        arrived(dx_ref.at[q], dx_recv.at[q])
    weights_sent(1)

    def drain(m, carry):
        home = m // 2
        mine = home == chip

        @pl.when(jnp.logical_not(last & mine))
        def _():
            sent(hout.at[m], h_send.at[m])

        @pl.when(jnp.logical_not(first & mine))
        def _():
            sent(gout.at[m], g_sent.at[m])
        return carry

    lax.fori_loop(0, n_chunk, drain, 0)
    for b in range(N_BLK):
        sent(w_all.at[core, b], w_fwd.at[b])
        sent(acc.at[1 - core, b], p_send.at[b])
        pushed(acc.at[core, b], dw_send.at[b], b, owner)
    for v in range(2):
        arrived(dwu_ref.at[v], dw_recv.at[0, v])
        arrived(dwd_ref.at[v], dw_recv.at[1, v])


def solution(mesh):
    tok_spec = P(('data', 'stage', 'inner'))
    up_spec = P(None, ('data', 'stage'), None, 'inner')
    down_spec = P(None, ('data', 'stage'), 'inner', None)

    def device_step(x_loc, g_loc, w_up, w_down):
        _, tokens, d = x_loc.shape
        ff = w_up.shape[3]
        rows = tokens // 2
        n_chunk = 2 * N_CHIP
        dma = pltpu.SemaphoreType.DMA
        hbm = pl.BlockSpec(memory_space=pl.ANY)
        flops = 7 * 2 * d * ff * N_BLK * n_chunk * rows
        y, dx, dwu, dwd = pl.pallas_call(
            kernel,
            out_shape=(
                jax.ShapeDtypeStruct((2, rows, d), BF16),
                jax.ShapeDtypeStruct((2, rows, d), BF16),
                jax.ShapeDtypeStruct((2, d, ff), F32),
                jax.ShapeDtypeStruct((2, ff, d), F32),
            ),
            in_specs=[hbm] * 4,
            out_specs=(hbm,) * 4,
            scratch_shapes=[
                pltpu.VMEM((2, N_BLK, d, ff), BF16),
                pltpu.VMEM((2, N_BLK, d, ff), F32),
                pltpu.VMEM((N_BLK, d, ff), F32),
                pltpu.VMEM((n_chunk, rows, d), BF16),
                pltpu.VMEM((n_chunk, rows, d), BF16),
                pltpu.VMEM((n_chunk, rows, d), BF16),
                pltpu.VMEM((n_chunk, rows, d), BF16),
                pltpu.VMEM((N_BLK, 2 * rows, ff), BF16),
                pltpu.VMEM((N_BLK, 2 * rows, ff), BF16),
                dma((2,)), dma((2,)), dma((2, 2)), dma((2, N_BLK)), dma((N_BLK,)),
                dma((n_chunk,)), dma((n_chunk,)), dma((n_chunk,)), dma((n_chunk,)),
                dma((2,)), dma((2,)), dma((N_BLK,)), dma((N_BLK,)), dma((N_BLK,)), dma((2, 2)),
            ],
            compiler_params=pltpu.CompilerParams(
                has_side_effects=True, vmem_limit_bytes=66 * 1000 * 1000),
            cost_estimate=pl.CostEstimate(flops=flops, bytes_accessed=40_000_000, transcendentals=0),
        )(x_loc.reshape(2, rows, d), g_loc.reshape(2, rows, d),
          w_up.reshape(2, d, ff), w_down.reshape(2, ff, d))
        return (y.reshape(x_loc.shape), dx.reshape(x_loc.shape),
                dwu.reshape(w_up.shape), dwd.reshape(w_down.shape))

    return jax.shard_map(device_step, mesh=mesh, in_specs=(tok_spec, tok_spec, up_spec, down_spec),
                         out_specs=(tok_spec, tok_spec, up_spec, down_spec), check_vma=False)
```

```python
import functools

import jax
import jax.numpy as jnp
from jax import lax
from jax.experimental import pallas as pl
from jax.experimental.pallas import tpu as pltpu
from jax.sharding import PartitionSpec as P

MESH = pl.DeviceIdType.MESH
F32 = jnp.float32
BF16 = jnp.bfloat16
N_CHIP = 8
N_BLK = 4


def gelu_only(z):
    return z * (0.5 * (1.0 + lax.erf(z * 0.7071067811865476)))


def gelu_pair(z):
    cdf = 0.5 * (1.0 + lax.erf(z * 0.7071067811865476))
    pdf = jnp.exp(-0.5 * z * z) * 0.3989422804014327
    return z * cdf, cdf + z * pdf


def dot_nn(a, b):
    return lax.dot_general(a, b, (((1,), (0,)), ((), ())), preferred_element_type=F32)


def dot_nt(a, b):
    return lax.dot_general(a, b, (((1,), (1,)), ((), ())), preferred_element_type=F32)


def dot_tn(a, b):
    return lax.dot_general(a, b, (((0,), (0,)), ((), ())), preferred_element_type=F32)


def chip_z(layer):
    return lax.rem(1 + (layer + 1) // 2, 4)


def chip_y(layer):
    return lax.rem(layer // 2, 2)


def kernel(x_ref, g_ref, wu_ref, wd_ref, y_ref, dx_ref, dwu_ref, dwd_ref,
           w_all, acc, pbuf, hbuf, hout, gbuf, gout, a_s, dz_s,
           x_send, g_send, w_send, w_recv, w_fwd, h_recv, g_recv, h_send, g_sent,
           y_recv, dx_recv, p_send, p_recv, dw_send, dw_recv):
    z = lax.axis_index("inner")
    s = lax.axis_index("stage")
    y = s // 2
    core = lax.rem(s, 2)
    par, half = lax.rem(z, 2), z // 2
    layer = (1 - y) * (5 - 5 * par - 4 * half + 8 * par * half) + y * (6 + par - 4 * half)
    n_chunk, rows, d = hbuf.shape
    partner = 2 * y + (1 - core)
    here = {"inner": z, "stage": s}

    def copy(src, dst, send, recv, dz, ds):
        return pltpu.make_async_remote_copy(
            src_ref=src, dst_ref=dst, send_sem=send, recv_sem=recv,
            device_id={"inner": dz, "stage": ds}, device_id_type=MESH)

    def arrived(slot, sem):
        copy(slot, slot, sem, sem, z, s).wait_recv()

    def sent(slot, sem):
        copy(slot, slot, sem, sem, z, s).wait_send()

    def push(src, dst, send, recv, dz, ds):
        same = (dz == z) & (ds == s)

        @pl.when(same)
        def _():
            pltpu.make_async_copy(src, dst, recv).start()

        @pl.when(jnp.logical_not(same))
        def _():
            copy(src, dst, send, recv, dz, ds).start()

    def pushed(src, send, dz, ds):
        @pl.when(jnp.logical_not((dz == z) & (ds == s)))
        def _():
            sent(src, send)

    def send_weights(v):
        tgt = chip_z(4 * v + s)
        push(wu_ref.at[v], w_all.at[0, z], w_send.at[v, 0], w_recv.at[0, z], tgt, 2 * y)
        push(wd_ref.at[v], w_all.at[1, z], w_send.at[v, 1], w_recv.at[1, z], tgt, 2 * y + 1)

    def weights_sent(v):
        tgt = chip_z(4 * v + s)
        pushed(wu_ref.at[v], w_send.at[v, 0], tgt, 2 * y)
        pushed(wd_ref.at[v], w_send.at[v, 1], tgt, 2 * y + 1)

    chip = 4 * y + z
    send_weights(0)
    for q in range(2):
        slot = 2 * chip + q
        push(x_ref.at[q], hbuf.at[slot], x_send.at[q], h_recv.at[slot], 1, core)
    for k in range(2):
        for b in range(N_BLK):
            acc[k, b] = jnp.zeros(acc.shape[2:], F32)
    early = layer < 4

    @pl.when(jnp.logical_not(early))
    def _():
        weights_sent(0)
        send_weights(1)

    for q in range(2):
        slot = 2 * chip + q
        push(g_ref.at[q], gbuf.at[slot], g_send.at[q], g_recv.at[slot], 1, 2 + core)
    for b in range(N_BLK):
        arrived(w_all.at[core, b], w_recv.at[core, b])
        copy(w_all.at[core, b], w_all.at[core, b], w_fwd.at[b], w_recv.at[core, b], z, partner).start()
    for b in range(N_BLK):
        arrived(w_all.at[1 - core, b], w_recv.at[1 - core, b])

    @pl.when(early)
    def _():
        weights_sent(0)
        send_weights(1)

    nxt, prv = layer + 1, layer - 1
    last, first = layer == N_CHIP - 1, layer == 0

    def forward(m):
        arrived(hbuf.at[m], h_recv.at[m])
        h = hbuf[m]
        out = h.astype(F32)
        branch = jnp.zeros((rows, d), F32)
        for b in range(N_BLK):
            a = gelu_only(dot_nn(h, w_all[0, b])).astype(BF16)
            branch = branch + dot_nn(a, w_all[1, b])
        hout[m] = (out + branch).astype(BF16)

        @pl.when(jnp.logical_not(last))
        def _():
            copy(hout.at[m], hbuf.at[m], h_send.at[m], h_recv.at[m],
                 chip_z(nxt), 2 * chip_y(nxt) + core).start()

        @pl.when(last)
        def _():
            home, q = m // 2, lax.rem(m, 2)
            push(hout.at[m], y_ref.at[q], h_send.at[m], y_recv.at[q],
                 lax.rem(home, 4), 2 * (home // 4) + core)

    def backward(m):
        q = lax.rem(m, 2)
        arrived(gbuf.at[m], g_recv.at[m])
        h = hbuf[m]
        g = gbuf[m]
        back = jnp.zeros((rows, d), F32)
        for b in range(N_BLK):
            act, grad = gelu_pair(dot_nn(h, w_all[0, b]))
            dz = (dot_nt(g, w_all[1, b]) * grad).astype(BF16)
            a_s[b, q] = act.astype(BF16)
            dz_s[b, q] = dz
            back = back + dot_nt(dz, w_all[0, b])
        gout[m] = (g.astype(F32) + back).astype(BF16)

        @pl.when(jnp.logical_not(first))
        def _():
            copy(gout.at[m], gbuf.at[m], g_sent.at[m], g_recv.at[m],
                 chip_z(prv), 2 * chip_y(prv) + core).start()

        @pl.when(first)
        def _():
            home = m // 2
            push(gout.at[m], dx_ref.at[q], g_sent.at[m], dx_recv.at[q],
                 lax.rem(home, 4), 2 * (home // 4) + core)

    def weight_grads(p):
        h2 = hbuf[pl.ds(2 * p, 2)].reshape(2 * rows, d)
        g2 = gbuf[pl.ds(2 * p, 2)].reshape(2 * rows, d)
        for b in range(N_BLK):
            acc[0, b] += dot_tn(h2, dz_s[b].reshape(2 * rows, -1))
            acc[1, b] += dot_tn(a_s[b].reshape(2 * rows, -1), g2)

    turn = 4 * (N_CHIP - 1) + 1

    def tick(t, carry):
        m_f = t - 2 * layer
        m_b = t - turn + 2 * layer

        @pl.when((m_f >= 0) & (m_f < n_chunk))
        def _():
            forward(m_f)

        @pl.when((m_b >= 0) & (m_b < n_chunk))
        def _():
            backward(m_b)

            @pl.when(lax.rem(m_b, 2) == 1)
            def _():
                weight_grads(m_b // 2)
        return carry

    lax.fori_loop(0, n_chunk + turn, tick, 0)

    order = [i + (1 - half) * (3 - 2 * i) for i in range(N_BLK)]
    for i, b in enumerate(order):
        copy(acc.at[1 - core, b], pbuf.at[i], p_send.at[i], p_recv.at[i], z, partner).start()
    virt = layer // 4
    owner = lax.rem(layer, 4)
    for i, b in enumerate(order):
        arrived(pbuf.at[i], p_recv.at[i])
        acc[core, b] += pbuf[i]

        @pl.when(core == 0)
        def _():
            push(acc.at[0, b], dwu_ref.at[virt], dw_send.at[i], dw_recv.at[0, virt], b, owner)

        @pl.when(core == 1)
        def _():
            push(acc.at[1, b], dwd_ref.at[virt], dw_send.at[i], dw_recv.at[1, virt], b, owner)

    for q in range(2):
        pushed(x_ref.at[q], x_send.at[q], 1, core)
        pushed(g_ref.at[q], g_send.at[q], 1, 2 + core)
        arrived(y_ref.at[q], y_recv.at[q])
        arrived(dx_ref.at[q], dx_recv.at[q])
    weights_sent(1)

    def drain(m, carry):
        home = m // 2
        mine = home == chip

        @pl.when(jnp.logical_not(last & mine))
        def _():
            sent(hout.at[m], h_send.at[m])

        @pl.when(jnp.logical_not(first & mine))
        def _():
            sent(gout.at[m], g_sent.at[m])
        return carry

    lax.fori_loop(0, n_chunk, drain, 0)
    for i, b in enumerate(order):
        sent(w_all.at[core, i], w_fwd.at[i])
        sent(acc.at[1 - core, b], p_send.at[i])
        pushed(acc.at[core, b], dw_send.at[i], b, owner)
    for v in range(2):
        arrived(dwu_ref.at[v], dw_recv.at[0, v])
        arrived(dwd_ref.at[v], dw_recv.at[1, v])


def solution(mesh):
    tok_spec = P(('data', 'stage', 'inner'))
    up_spec = P(None, ('data', 'stage'), None, 'inner')
    down_spec = P(None, ('data', 'stage'), 'inner', None)

    def device_step(x_loc, g_loc, w_up, w_down):
        _, tokens, d = x_loc.shape
        ff = w_up.shape[3]
        rows = tokens // 2
        n_chunk = 2 * N_CHIP
        dma = pltpu.SemaphoreType.DMA
        hbm = pl.BlockSpec(memory_space=pl.ANY)
        flops = 7 * 2 * d * ff * N_BLK * n_chunk * rows
        y, dx, dwu, dwd = pl.pallas_call(
            kernel,
            out_shape=(
                jax.ShapeDtypeStruct((2, rows, d), BF16),
                jax.ShapeDtypeStruct((2, rows, d), BF16),
                jax.ShapeDtypeStruct((2, d, ff), F32),
                jax.ShapeDtypeStruct((2, ff, d), F32),
            ),
            in_specs=[hbm] * 4,
            out_specs=(hbm,) * 4,
            scratch_shapes=[
                pltpu.VMEM((2, N_BLK, d, ff), BF16),
                pltpu.VMEM((2, N_BLK, d, ff), F32),
                pltpu.VMEM((N_BLK, d, ff), F32),
                pltpu.VMEM((n_chunk, rows, d), BF16),
                pltpu.VMEM((n_chunk, rows, d), BF16),
                pltpu.VMEM((n_chunk, rows, d), BF16),
                pltpu.VMEM((n_chunk, rows, d), BF16),
                pltpu.VMEM((N_BLK, 2, rows, ff), BF16),
                pltpu.VMEM((N_BLK, 2, rows, ff), BF16),
                dma((2,)), dma((2,)), dma((2, 2)), dma((2, N_BLK)), dma((N_BLK,)),
                dma((n_chunk,)), dma((n_chunk,)), dma((n_chunk,)), dma((n_chunk,)),
                dma((2,)), dma((2,)), dma((N_BLK,)), dma((N_BLK,)), dma((N_BLK,)), dma((2, 2)),
            ],
            compiler_params=pltpu.CompilerParams(
                has_side_effects=True, vmem_limit_bytes=66 * 1000 * 1000),
            cost_estimate=pl.CostEstimate(flops=flops, bytes_accessed=40_000_000, transcendentals=0),
        )(x_loc.reshape(2, rows, d), g_loc.reshape(2, rows, d),
          w_up.reshape(2, d, ff), w_down.reshape(2, ff, d))
        return (y.reshape(x_loc.shape), dx.reshape(x_loc.shape),
                dwu.reshape(w_up.shape), dwd.reshape(w_down.shape))

    return jax.shard_map(device_step, mesh=mesh, in_specs=(tok_spec, tok_spec, up_spec, down_spec),
                         out_specs=(tok_spec, tok_spec, up_spec, down_spec), check_vma=False)
```

```python
import functools

import jax
import jax.numpy as jnp
from jax import lax
from jax.experimental import pallas as pl
from jax.experimental.pallas import tpu as pltpu
from jax.sharding import PartitionSpec as P

MESH = pl.DeviceIdType.MESH
F32 = jnp.float32
BF16 = jnp.bfloat16
N_CHIP = 8
N_BLK = 4


def gelu_only(z):
    return z * (0.5 * (1.0 + lax.erf(z * 0.7071067811865476)))


def gelu_pair(z):
    cdf = 0.5 * (1.0 + lax.erf(z * 0.7071067811865476))
    pdf = jnp.exp(-0.5 * z * z) * 0.3989422804014327
    return z * cdf, cdf + z * pdf


def dot_nn(a, b):
    return lax.dot_general(a, b, (((1,), (0,)), ((), ())), preferred_element_type=F32)


def dot_nt(a, b):
    return lax.dot_general(a, b, (((1,), (1,)), ((), ())), preferred_element_type=F32)


def dot_tn(a, b):
    return lax.dot_general(a, b, (((0,), (0,)), ((), ())), preferred_element_type=F32)


def chip_z(layer):
    return lax.rem(1 + (layer + 1) // 2, 4)


def chip_y(layer):
    return lax.rem(layer // 2, 2)


def kernel(x_ref, g_ref, wu_ref, wd_ref, y_ref, dx_ref, dwu_ref, dwd_ref,
           w_all, acc, pbuf, hbuf, hout, gbuf, gout, a_s, dz_s,
           x_send, g_send, w_send, w_recv, w_fwd, h_recv, g_recv, h_send, g_sent,
           y_recv, dx_recv, p_send, p_recv, dw_send, dw_recv, go):
    z = lax.axis_index("inner")
    s = lax.axis_index("stage")
    y = s // 2
    core = lax.rem(s, 2)
    par, half = lax.rem(z, 2), z // 2
    layer = (1 - y) * (5 - 5 * par - 4 * half + 8 * par * half) + y * (6 + par - 4 * half)
    n_chunk, rows, d = hbuf.shape
    partner = 2 * y + (1 - core)

    def copy(src, dst, send, recv, dz, ds):
        return pltpu.make_async_remote_copy(
            src_ref=src, dst_ref=dst, send_sem=send, recv_sem=recv,
            device_id={"inner": dz, "stage": ds}, device_id_type=MESH)

    def arrived(slot, sem):
        copy(slot, slot, sem, sem, z, s).wait_recv()

    def sent(slot, sem):
        copy(slot, slot, sem, sem, z, s).wait_send()

    def push(src, dst, send, recv, dz, ds):
        same = (dz == z) & (ds == s)

        @pl.when(same)
        def _():
            pltpu.make_async_copy(src, dst, recv).start()

        @pl.when(jnp.logical_not(same))
        def _():
            copy(src, dst, send, recv, dz, ds).start()

    def pushed(src, send, dz, ds):
        @pl.when(jnp.logical_not((dz == z) & (ds == s)))
        def _():
            sent(src, send)

    def send_weights(v):
        tgt = chip_z(4 * v + s)
        push(wu_ref.at[v], w_all.at[0, z], w_send.at[v, 0], w_recv.at[0, z], tgt, 2 * y)
        push(wd_ref.at[v], w_all.at[1, z], w_send.at[v, 1], w_recv.at[1, z], tgt, 2 * y + 1)

    def weights_sent(v):
        tgt = chip_z(4 * v + s)
        pushed(wu_ref.at[v], w_send.at[v, 0], tgt, 2 * y)
        pushed(wd_ref.at[v], w_send.at[v, 1], tgt, 2 * y + 1)

    chip = 4 * half + 2 * y + par
    send_weights(0)
    for q in range(2):
        slot = 2 * chip + q
        push(x_ref.at[q], hbuf.at[slot], x_send.at[q], h_recv.at[slot], 1, core)
    for k in range(2):
        for b in range(N_BLK):
            acc[k, b] = jnp.zeros(acc.shape[2:], F32)
    early = (y == 0) & (layer < 4)
    late = (y == 0) & (layer >= 4)

    @pl.when(y == 1)
    def _():
        weights_sent(0)
        send_weights(1)

    for q in range(2):
        slot = 2 * chip + q
        push(g_ref.at[q], gbuf.at[slot], g_send.at[q], g_recv.at[slot], 1, 2 + core)
    @pl.when(late)
    def _():
        weights_sent(0)
        pl.semaphore_wait(go, 1)
        send_weights(1)

    for b in range(N_BLK):
        arrived(w_all.at[core, b], w_recv.at[core, b])
        copy(w_all.at[core, b], w_all.at[core, b], w_fwd.at[b], w_recv.at[core, b], z, partner).start()
    for b in range(N_BLK):
        arrived(w_all.at[1 - core, b], w_recv.at[1 - core, b])

    @pl.when(early)
    def _():
        pl.semaphore_signal(go, inc=1, device_id={"inner": lax.rem(z + 2, 4), "stage": s},
                            device_id_type=MESH)
        weights_sent(0)
        send_weights(1)

    nxt, prv = layer + 1, layer - 1
    last, first = layer == N_CHIP - 1, layer == 0

    def forward(m):
        arrived(hbuf.at[m], h_recv.at[m])
        h = hbuf[m]
        out = h.astype(F32)
        branch = jnp.zeros((rows, d), F32)
        for b in range(N_BLK):
            a = gelu_only(dot_nn(h, w_all[0, b])).astype(BF16)
            branch = branch + dot_nn(a, w_all[1, b])
        hout[m] = (out + branch).astype(BF16)

        @pl.when(jnp.logical_not(last))
        def _():
            copy(hout.at[m], hbuf.at[m], h_send.at[m], h_recv.at[m],
                 chip_z(nxt), 2 * chip_y(nxt) + core).start()

        @pl.when(last)
        def _():
            home, q = m // 2, lax.rem(m, 2)
            push(hout.at[m], y_ref.at[q], h_send.at[m], y_recv.at[q],
                 2 * (home // 4) + lax.rem(home, 2), 2 * lax.rem(home // 2, 2) + core)

    def backward(m):
        q = lax.rem(m, 2)
        arrived(gbuf.at[m], g_recv.at[m])
        h = hbuf[m]
        g = gbuf[m]
        back = jnp.zeros((rows, d), F32)
        for b in range(N_BLK):
            act, grad = gelu_pair(dot_nn(h, w_all[0, b]))
            dz = (dot_nt(g, w_all[1, b]) * grad).astype(BF16)
            a_s[b, q] = act.astype(BF16)
            dz_s[b, q] = dz
            back = back + dot_nt(dz, w_all[0, b])
        gout[m] = (g.astype(F32) + back).astype(BF16)

        @pl.when(jnp.logical_not(first))
        def _():
            copy(gout.at[m], gbuf.at[m], g_sent.at[m], g_recv.at[m],
                 chip_z(prv), 2 * chip_y(prv) + core).start()

        @pl.when(first)
        def _():
            home = m // 2
            push(gout.at[m], dx_ref.at[q], g_sent.at[m], dx_recv.at[q],
                 2 * (home // 4) + lax.rem(home, 2), 2 * lax.rem(home // 2, 2) + core)

    def weight_grads(p):
        h2 = hbuf[pl.ds(2 * p, 2)].reshape(2 * rows, d)
        g2 = gbuf[pl.ds(2 * p, 2)].reshape(2 * rows, d)
        for b in range(N_BLK):
            acc[0, b] += dot_tn(h2, dz_s[b].reshape(2 * rows, -1))
            acc[1, b] += dot_tn(a_s[b].reshape(2 * rows, -1), g2)

    turn = 4 * (N_CHIP - 1) + 1

    def tick(t, carry):
        m_f = t - 2 * layer
        m_b = t - turn + 2 * layer

        @pl.when((m_f >= 0) & (m_f < n_chunk))
        def _():
            forward(m_f)

        @pl.when((m_b >= 0) & (m_b < n_chunk))
        def _():
            backward(m_b)

            @pl.when(lax.rem(m_b, 2) == 1)
            def _():
                weight_grads(m_b // 2)
        return carry

    lax.fori_loop(0, n_chunk + turn, tick, 0)

    order = [i + (1 - half) * (3 - 2 * i) for i in range(N_BLK)]
    for i, b in enumerate(order):
        copy(acc.at[1 - core, b], pbuf.at[i], p_send.at[i], p_recv.at[i], z, partner).start()
    virt = layer // 4
    owner = lax.rem(layer, 4)
    for i, b in enumerate(order):
        arrived(pbuf.at[i], p_recv.at[i])
        acc[core, b] += pbuf[i]

        @pl.when(core == 0)
        def _():
            push(acc.at[0, b], dwu_ref.at[virt], dw_send.at[i], dw_recv.at[0, virt], b, owner)

        @pl.when(core == 1)
        def _():
            push(acc.at[1, b], dwd_ref.at[virt], dw_send.at[i], dw_recv.at[1, virt], b, owner)

    for q in range(2):
        pushed(x_ref.at[q], x_send.at[q], 1, core)
        pushed(g_ref.at[q], g_send.at[q], 1, 2 + core)
        arrived(y_ref.at[q], y_recv.at[q])
        arrived(dx_ref.at[q], dx_recv.at[q])
    weights_sent(1)

    def drain(m, carry):
        home = m // 2
        mine = home == chip

        @pl.when(jnp.logical_not(last & mine))
        def _():
            sent(hout.at[m], h_send.at[m])

        @pl.when(jnp.logical_not(first & mine))
        def _():
            sent(gout.at[m], g_sent.at[m])
        return carry

    lax.fori_loop(0, n_chunk, drain, 0)
    for i, b in enumerate(order):
        sent(w_all.at[core, i], w_fwd.at[i])
        sent(acc.at[1 - core, b], p_send.at[i])
        pushed(acc.at[core, b], dw_send.at[i], b, owner)
    for v in range(2):
        arrived(dwu_ref.at[v], dw_recv.at[0, v])
        arrived(dwd_ref.at[v], dw_recv.at[1, v])


def solution(mesh):
    tok_spec = P(('data', 'stage', 'inner'))
    up_spec = P(None, ('data', 'stage'), None, 'inner')
    down_spec = P(None, ('data', 'stage'), 'inner', None)

    def device_step(x_loc, g_loc, w_up, w_down):
        _, tokens, d = x_loc.shape
        ff = w_up.shape[3]
        rows = tokens // 2
        n_chunk = 2 * N_CHIP
        dma = pltpu.SemaphoreType.DMA
        hbm = pl.BlockSpec(memory_space=pl.ANY)
        flops = 7 * 2 * d * ff * N_BLK * n_chunk * rows
        y, dx, dwu, dwd = pl.pallas_call(
            kernel,
            out_shape=(
                jax.ShapeDtypeStruct((2, rows, d), BF16),
                jax.ShapeDtypeStruct((2, rows, d), BF16),
                jax.ShapeDtypeStruct((2, d, ff), F32),
                jax.ShapeDtypeStruct((2, ff, d), F32),
            ),
            in_specs=[hbm] * 4,
            out_specs=(hbm,) * 4,
            scratch_shapes=[
                pltpu.VMEM((2, N_BLK, d, ff), BF16),
                pltpu.VMEM((2, N_BLK, d, ff), F32),
                pltpu.VMEM((N_BLK, d, ff), F32),
                pltpu.VMEM((n_chunk, rows, d), BF16),
                pltpu.VMEM((n_chunk, rows, d), BF16),
                pltpu.VMEM((n_chunk, rows, d), BF16),
                pltpu.VMEM((n_chunk, rows, d), BF16),
                pltpu.VMEM((N_BLK, 2, rows, ff), BF16),
                pltpu.VMEM((N_BLK, 2, rows, ff), BF16),
                dma((2,)), dma((2,)), dma((2, 2)), dma((2, N_BLK)), dma((N_BLK,)),
                dma((n_chunk,)), dma((n_chunk,)), dma((n_chunk,)), dma((n_chunk,)),
                dma((2,)), dma((2,)), dma((N_BLK,)), dma((N_BLK,)), dma((N_BLK,)), dma((2, 2)),
                pltpu.SemaphoreType.REGULAR,
            ],
            compiler_params=pltpu.CompilerParams(
                has_side_effects=True, vmem_limit_bytes=66 * 1000 * 1000),
            cost_estimate=pl.CostEstimate(flops=flops, bytes_accessed=40_000_000, transcendentals=0),
        )(x_loc.reshape(2, rows, d), g_loc.reshape(2, rows, d),
          w_up.reshape(2, d, ff), w_down.reshape(2, ff, d))
        return (y.reshape(x_loc.shape), dx.reshape(x_loc.shape),
                dwu.reshape(w_up.shape), dwd.reshape(w_down.shape))

    return jax.shard_map(device_step, mesh=mesh, in_specs=(tok_spec, tok_spec, up_spec, down_spec),
                         out_specs=(tok_spec, tok_spec, up_spec, down_spec), check_vma=False)
```

```python
import functools

import jax
import jax.numpy as jnp
from jax import lax
from jax.experimental import pallas as pl
from jax.experimental.pallas import tpu as pltpu
from jax.sharding import PartitionSpec as P

MESH = pl.DeviceIdType.MESH
F32 = jnp.float32
BF16 = jnp.bfloat16
N_CHIP = 8
N_BLK = 4


def gelu_only(z):
    return z * (0.5 * (1.0 + lax.erf(z * 0.7071067811865476)))


def gelu_pair(z):
    cdf = 0.5 * (1.0 + lax.erf(z * 0.7071067811865476))
    pdf = jnp.exp(-0.5 * z * z) * 0.3989422804014327
    return z * cdf, cdf + z * pdf


def dot_nn(a, b):
    return lax.dot_general(a, b, (((1,), (0,)), ((), ())), preferred_element_type=F32)


def dot_nt(a, b):
    return lax.dot_general(a, b, (((1,), (1,)), ((), ())), preferred_element_type=F32)


def dot_tn(a, b):
    return lax.dot_general(a, b, (((0,), (0,)), ((), ())), preferred_element_type=F32)


def chip_z(layer):
    return lax.rem(1 + (layer + 1) // 2, 4)


def chip_y(layer):
    return lax.rem(layer // 2, 2)


def kernel(x_ref, g_ref, wu_ref, wd_ref, y_ref, dx_ref, dwu_ref, dwd_ref,
           w_all, acc, pbuf, hbuf, hout, gbuf, gout, a_s, dz_s,
           x_send, g_send, w_send, w_recv, w_fwd, h_recv, g_recv, h_send, g_sent,
           y_recv, dx_recv, p_send, p_recv, dw_send, dw_recv):
    z = lax.axis_index("inner")
    s = lax.axis_index("stage")
    y = s // 2
    core = lax.rem(s, 2)
    par, half = lax.rem(z, 2), z // 2
    layer = (1 - y) * (5 - 5 * par - 4 * half + 8 * par * half) + y * (6 + par - 4 * half)
    n_chunk, rows, d = hbuf.shape
    partner = 2 * y + (1 - core)

    def copy(src, dst, send, recv, dz, ds):
        return pltpu.make_async_remote_copy(
            src_ref=src, dst_ref=dst, send_sem=send, recv_sem=recv,
            device_id={"inner": dz, "stage": ds}, device_id_type=MESH)

    def arrived(slot, sem):
        copy(slot, slot, sem, sem, z, s).wait_recv()

    def sent(slot, sem):
        copy(slot, slot, sem, sem, z, s).wait_send()

    def push(src, dst, send, recv, dz, ds):
        same = (dz == z) & (ds == s)

        @pl.when(same)
        def _():
            pltpu.make_async_copy(src, dst, recv).start()

        @pl.when(jnp.logical_not(same))
        def _():
            copy(src, dst, send, recv, dz, ds).start()

    def pushed(src, send, dz, ds):
        @pl.when(jnp.logical_not((dz == z) & (ds == s)))
        def _():
            sent(src, send)

    def send_weights(v):
        tgt = chip_z(4 * v + s)
        push(wu_ref.at[v], w_all.at[0, z], w_send.at[v, 0], w_recv.at[0, z], tgt, 2 * y)
        push(wd_ref.at[v], w_all.at[1, z], w_send.at[v, 1], w_recv.at[1, z], tgt, 2 * y + 1)

    def weights_sent(v):
        tgt = chip_z(4 * v + s)
        pushed(wu_ref.at[v], w_send.at[v, 0], tgt, 2 * y)
        pushed(wd_ref.at[v], w_send.at[v, 1], tgt, 2 * y + 1)

    chip = 4 * half + 2 * y + par
    send_weights(0)
    for q in range(2):
        slot = 2 * chip + q
        push(x_ref.at[q], hbuf.at[slot], x_send.at[q], h_recv.at[slot], 1, core)
    for k in range(2):
        for b in range(N_BLK):
            acc[k, b] = jnp.zeros(acc.shape[2:], F32)
    weights_sent(0)
    send_weights(1)
    for q in range(2):
        slot = 2 * chip + q
        push(g_ref.at[q], gbuf.at[slot], g_send.at[q], g_recv.at[slot], 1, 2 + core)

    for b in range(N_BLK):
        arrived(w_all.at[core, b], w_recv.at[core, b])
        copy(w_all.at[core, b], w_all.at[core, b], w_fwd.at[b], w_recv.at[core, b], z, partner).start()
    for b in range(N_BLK):
        arrived(w_all.at[1 - core, b], w_recv.at[1 - core, b])

    nxt, prv = layer + 1, layer - 1
    last, first = layer == N_CHIP - 1, layer == 0

    def forward(m):
        arrived(hbuf.at[m], h_recv.at[m])
        h = hbuf[m]
        out = h.astype(F32)
        branch = jnp.zeros((rows, d), F32)
        for b in range(N_BLK):
            a = gelu_only(dot_nn(h, w_all[0, b])).astype(BF16)
            branch = branch + dot_nn(a, w_all[1, b])
        hout[m] = (out + branch).astype(BF16)

        @pl.when(jnp.logical_not(last))
        def _():
            copy(hout.at[m], hbuf.at[m], h_send.at[m], h_recv.at[m],
                 chip_z(nxt), 2 * chip_y(nxt) + core).start()

        @pl.when(last)
        def _():
            home, q = m // 2, lax.rem(m, 2)
            push(hout.at[m], y_ref.at[q], h_send.at[m], y_recv.at[q],
                 2 * (home // 4) + lax.rem(home, 2), 2 * lax.rem(home // 2, 2) + core)

    def backward(m):
        q = lax.rem(m, 2)
        arrived(gbuf.at[m], g_recv.at[m])
        h = hbuf[m]
        g = gbuf[m]
        back = jnp.zeros((rows, d), F32)
        for b in range(N_BLK):
            act, grad = gelu_pair(dot_nn(h, w_all[0, b]))
            dz = (dot_nt(g, w_all[1, b]) * grad).astype(BF16)
            a_s[b, q] = act.astype(BF16)
            dz_s[b, q] = dz
            back = back + dot_nt(dz, w_all[0, b])
        gout[m] = (g.astype(F32) + back).astype(BF16)

        @pl.when(jnp.logical_not(first))
        def _():
            copy(gout.at[m], gbuf.at[m], g_sent.at[m], g_recv.at[m],
                 chip_z(prv), 2 * chip_y(prv) + core).start()

        @pl.when(first)
        def _():
            home = m // 2
            push(gout.at[m], dx_ref.at[q], g_sent.at[m], dx_recv.at[q],
                 2 * (home // 4) + lax.rem(home, 2), 2 * lax.rem(home // 2, 2) + core)

    def weight_grads(p):
        h2 = hbuf[pl.ds(2 * p, 2)].reshape(2 * rows, d)
        g2 = gbuf[pl.ds(2 * p, 2)].reshape(2 * rows, d)
        for b in range(N_BLK):
            acc[0, b] += dot_tn(h2, dz_s[b].reshape(2 * rows, -1))
            acc[1, b] += dot_tn(a_s[b].reshape(2 * rows, -1), g2)

    turn = 4 * (N_CHIP - 1) + 1

    def tick(t, carry):
        m_f = t - 2 * layer
        m_b = t - turn + 2 * layer

        @pl.when((m_f >= 0) & (m_f < n_chunk))
        def _():
            forward(m_f)

        @pl.when((m_b >= 0) & (m_b < n_chunk))
        def _():
            backward(m_b)

            @pl.when(lax.rem(m_b, 2) == 1)
            def _():
                weight_grads(m_b // 2)
        return carry

    lax.fori_loop(0, n_chunk + turn, tick, 0)

    order = [i + (1 - half) * (3 - 2 * i) for i in range(N_BLK)]
    for i, b in enumerate(order):
        copy(acc.at[1 - core, b], pbuf.at[i], p_send.at[i], p_recv.at[i], z, partner).start()
    virt = layer // 4
    owner = lax.rem(layer, 4)
    for i, b in enumerate(order):
        arrived(pbuf.at[i], p_recv.at[i])
        acc[core, b] += pbuf[i]

        @pl.when(core == 0)
        def _():
            push(acc.at[0, b], dwu_ref.at[virt], dw_send.at[i], dw_recv.at[0, virt], b, owner)

        @pl.when(core == 1)
        def _():
            push(acc.at[1, b], dwd_ref.at[virt], dw_send.at[i], dw_recv.at[1, virt], b, owner)

    for q in range(2):
        pushed(x_ref.at[q], x_send.at[q], 1, core)
        pushed(g_ref.at[q], g_send.at[q], 1, 2 + core)
        arrived(y_ref.at[q], y_recv.at[q])
        arrived(dx_ref.at[q], dx_recv.at[q])
    weights_sent(1)

    def drain(m, carry):
        home = m // 2
        mine = home == chip

        @pl.when(jnp.logical_not(last & mine))
        def _():
            sent(hout.at[m], h_send.at[m])

        @pl.when(jnp.logical_not(first & mine))
        def _():
            sent(gout.at[m], g_sent.at[m])
        return carry

    lax.fori_loop(0, n_chunk, drain, 0)
    for i, b in enumerate(order):
        sent(w_all.at[core, i], w_fwd.at[i])
        sent(acc.at[1 - core, b], p_send.at[i])
        pushed(acc.at[core, b], dw_send.at[i], b, owner)
    for v in range(2):
        arrived(dwu_ref.at[v], dw_recv.at[0, v])
        arrived(dwd_ref.at[v], dw_recv.at[1, v])


def solution(mesh):
    tok_spec = P(('data', 'stage', 'inner'))
    up_spec = P(None, ('data', 'stage'), None, 'inner')
    down_spec = P(None, ('data', 'stage'), 'inner', None)

    def device_step(x_loc, g_loc, w_up, w_down):
        _, tokens, d = x_loc.shape
        ff = w_up.shape[3]
        rows = tokens // 2
        n_chunk = 2 * N_CHIP
        dma = pltpu.SemaphoreType.DMA
        hbm = pl.BlockSpec(memory_space=pl.ANY)
        flops = 7 * 2 * d * ff * N_BLK * n_chunk * rows
        y, dx, dwu, dwd = pl.pallas_call(
            kernel,
            out_shape=(
                jax.ShapeDtypeStruct((2, rows, d), BF16),
                jax.ShapeDtypeStruct((2, rows, d), BF16),
                jax.ShapeDtypeStruct((2, d, ff), F32),
                jax.ShapeDtypeStruct((2, ff, d), F32),
            ),
            in_specs=[hbm] * 4,
            out_specs=(hbm,) * 4,
            scratch_shapes=[
                pltpu.VMEM((2, N_BLK, d, ff), BF16),
                pltpu.VMEM((2, N_BLK, d, ff), F32),
                pltpu.VMEM((N_BLK, d, ff), F32),
                pltpu.VMEM((n_chunk, rows, d), BF16),
                pltpu.VMEM((n_chunk, rows, d), BF16),
                pltpu.VMEM((n_chunk, rows, d), BF16),
                pltpu.VMEM((n_chunk, rows, d), BF16),
                pltpu.VMEM((N_BLK, 2, rows, ff), BF16),
                pltpu.VMEM((N_BLK, 2, rows, ff), BF16),
                dma((2,)), dma((2,)), dma((2, 2)), dma((2, N_BLK)), dma((N_BLK,)),
                dma((n_chunk,)), dma((n_chunk,)), dma((n_chunk,)), dma((n_chunk,)),
                dma((2,)), dma((2,)), dma((N_BLK,)), dma((N_BLK,)), dma((N_BLK,)), dma((2, 2)),
            ],
            compiler_params=pltpu.CompilerParams(
                has_side_effects=True, vmem_limit_bytes=66 * 1000 * 1000),
            cost_estimate=pl.CostEstimate(flops=flops, bytes_accessed=40_000_000, transcendentals=0),
        )(x_loc.reshape(2, rows, d), g_loc.reshape(2, rows, d),
          w_up.reshape(2, d, ff), w_down.reshape(2, ff, d))
        return (y.reshape(x_loc.shape), dx.reshape(x_loc.shape),
                dwu.reshape(w_up.shape), dwd.reshape(w_down.shape))

    return jax.shard_map(device_step, mesh=mesh, in_specs=(tok_spec, tok_spec, up_spec, down_spec),
                         out_specs=(tok_spec, tok_spec, up_spec, down_spec), check_vma=False)
```
